32 devices in a mesh: row: 4 (over y, core), col: 8 (over z, x).
Axes of the slice: x: 2, y: 2, z: 4, core: 2. Of those that a mesh axis runs over, the one named last changes fastest.
Arguments:
- lower_inverse: float32 [4, 8, 1024, 1024], P('row', 'col'), may hold values from -1 to 2, as said below
- upper_inverse: float32 [4, 8, 1024, 1024], P('row', 'col'), may hold values from -1 to 2, as said below
- left_coupling: bfloat16 [4, 8, 512, 1024], P('row', 'col'), may hold values from -0.1875 to 0.1875
- right_pieces: float32 [8, 1024, 2048], P('col', None, 'row'), may hold values from -6 to 6
- interface_block: int32 [4, 8, 4], P('row', 'col'), may hold values from 0 to 7, all different within a row
- a_gg: float32 [4, 1024, 2048], P('row', 'col'), may hold values from -6 to 6
- panel_order: int32 [4], replicated, may hold values from 0 to 3, each once
Outputs:
- schur: float32 [4, 1024, 2048], P('row', 'col')
The draws below stay inside these ranges and needn't reach their ends.
Inputs may be any that keep to these rules, and one draw needn't show every extreme that they name: `interface_block`: the 4 block ids of one subdomain are distinct. `panel_order`: A permutation of the column blocks. `lower_inverse`: lower triangular, diagonal between 1 and 2. `upper_inverse`: upper triangular, diagonal between 1 and 2.
All inputs are finite; a program needn't handle non-finite values.
Results may differ from the reference program's by a relative error of at most 0.0028.
Values sent between devices are 32-bit elements; how exact they have to be, the bound alone decides.
A program may use at most 128 MiB of HBM per device.

```python
import jax
import jax.numpy as jnp
from jax import lax

NI = 1024
PW = 2048
WB = 128
KB = 4
PR = 1024
N_ROW = 4
N_COL = 8


def make_factor(key, below):
    first_key, second_key = jax.random.split(key)
    shape = (N_ROW, N_COL, NI, NI)
    spread = jnp.clip(jax.random.normal(first_key, shape, jnp.float32), -6.0, 6.0) * (0.5 / NI ** 0.5)
    diagonal = jax.random.uniform(second_key, (N_ROW, N_COL, NI), jnp.float32, 1.0, 2.0)
    rows = lax.broadcasted_iota(jnp.int32, (NI, NI), 0)
    cols = lax.broadcasted_iota(jnp.int32, (NI, NI), 1)
    if below:
        keep = rows > cols
    else:
        keep = rows < cols
    ones = (rows == cols).astype(jnp.float32)
    return jnp.where(keep, spread, 0.0) + diagonal[..., None] * ones


def draw_lower_inverse(key, part):
    return make_factor(jax.random.fold_in(key, 11), True)


def draw_upper_inverse(key, part):
    return make_factor(jax.random.fold_in(key, 23), False)


def steps_of(stream_key, shape, cuts, least, top_value):
    def one(dim, shards_of):
        steps = jax.random.uniform(jax.random.fold_in(jax.random.fold_in(stream_key, 6), dim), (shards_of,), jnp.float32, least / len(cuts), top_value / len(cuts))
        return jnp.repeat(jnp.exp(steps), shape[dim] // shards_of).reshape((-1,) + (1,) * (len(shape) - dim - 1))

    loudness = one(*cuts[0])
    for cut in cuts[1:]:
        loudness = loudness * one(*cut)
    return loudness


def different_ones(own_key, rows, number_of, top, lift):
    sequence = jax.random.permutation(jax.random.fold_in(own_key, 1), number_of)
    boost = sequence
    for power in range(3):
        boost = boost * boost // number_of
    boost = boost * lift // number_of
    tickets = jax.random.randint(jax.random.fold_in(own_key, 2), (rows, number_of), 0, 4096) + boost
    holders = jax.random.permutation(jax.random.fold_in(own_key, 3), rows)[jnp.arange(number_of) % rows]
    tickets = jnp.where(jnp.arange(rows)[:, None] == holders[None, :], 1 << 14, tickets)
    priority = tickets * number_of + jnp.arange(number_of)
    return lax.top_k(priority.astype(jnp.int32), top)[1].astype(jnp.int32)


def noise(stream_key, shape, scale, bound, cuts=(), held_as=jnp.bfloat16):
    array = scale * jax.random.normal(stream_key, shape, jnp.float32)
    if cuts:
        array = array * steps_of(stream_key, shape, cuts, -0.22, 0.18)
    return jnp.clip(array, -bound, bound).astype(held_as)


def setup_inputs(seed: int = 0) -> dict:
    streams_of = jax.random.split(jax.random.key(seed), 8)
    lower_inverse = draw_lower_inverse(jax.random.fold_in(streams_of[7], 71), 0)
    upper_inverse = draw_upper_inverse(jax.random.fold_in(streams_of[7], 71), 0)
    left_coupling = noise(streams_of[2], (N_ROW, N_COL, KB * WB, NI), NI ** -0.5, 0.1875, ((0, 4), (1, 8)))
    right_pieces = noise(streams_of[3], (N_COL, NI, PW), 1.0, 6.0, ((0, 8), (2, 4)), jnp.float32)
    interface_block = different_ones(streams_of[4], N_ROW * N_COL, N_COL, KB, 0).reshape((N_ROW, N_COL, KB))
    a_gg = noise(streams_of[5], (N_ROW, PR, PW), 1.0, 6.0, ((0, 4), (1, 8)), jnp.float32)
    panel_order = jax.random.permutation(streams_of[6], N_ROW).astype(jnp.int32)
    return {"lower_inverse": lower_inverse, "upper_inverse": upper_inverse, "left_coupling": left_coupling, "right_pieces": right_pieces, "interface_block": interface_block, "a_gg": a_gg, "panel_order": panel_order}


def column_order(panel_order):
    length = panel_order.shape[0]
    positions = jnp.arange(length, dtype=jnp.int32)
    hits = (panel_order[:, None] == positions[None, :]).astype(jnp.int32)
    return jnp.sum(hits * positions[:, None], axis=0).astype(jnp.int32)


def couple(lower_mat, upper_mat, left_mat, panel):
    halfway = jnp.dot(lower_mat, panel, precision=lax.Precision.HIGHEST, preferred_element_type=jnp.float32)
    solved = jnp.dot(upper_mat, halfway, precision=lax.Precision.HIGHEST, preferred_element_type=jnp.float32)
    solved = solved.astype(jnp.bfloat16)
    return jnp.dot(left_mat, solved, preferred_element_type=jnp.float32)


def place_rows(coupled, block_ids, first_block, block_total):
    block_count = block_ids.shape[0]
    block_rows = coupled.shape[0] // block_count
    targets = first_block + jnp.arange(block_total, dtype=jnp.int32)
    placed = (block_ids[:, None] == targets[None, :]).astype(jnp.float32)
    shaped = coupled.reshape(block_count, block_rows, coupled.shape[1])
    spread = jnp.einsum("kb,kwp->bwp", placed, shaped, precision=lax.Precision.HIGHEST)
    return spread.reshape(block_total * block_rows, coupled.shape[1])


def reference(lower_inverse, upper_inverse, left_coupling, right_pieces, interface_block, a_gg, panel_order):
    row_count = lower_inverse.shape[0]
    col_count = lower_inverse.shape[1]
    inner = right_pieces.shape[1]
    width_piece = right_pieces.shape[2] // row_count
    order = column_order(panel_order)
    panels = right_pieces.reshape(col_count, inner, row_count, width_piece)[:, :, order, :]
    panels = panels.reshape(col_count, inner, row_count * width_piece)

    def one_row(row_args):
        lowers, uppers, lefts, blocks, base = row_args

        def add_one(summed, item):
            lower_mat, upper_mat, left_mat, block_ids, panel = item
            coupled = couple(lower_mat, upper_mat, left_mat, panel)
            return summed + place_rows(coupled, block_ids, 0, col_count), None

        summed, _ = lax.scan(add_one, jnp.zeros(base.shape, jnp.float32), (lowers, uppers, lefts, blocks, panels))
        return base - summed

    return lax.map(one_row, (lower_inverse, upper_inverse, left_coupling, interface_block, a_gg))
```

```python
import functools

import jax
import jax.numpy as jnp
import numpy as np
from jax import lax
from jax.experimental import pallas as pl
from jax.experimental.pallas import tpu as pltpu
from jax.sharding import PartitionSpec as P

MESH = pl.DeviceIdType.MESH
GROUP_WIDTH = 512
TILE = 256
VMEM_LIMIT = 60 * 1024 * 1024


def ring_order(length):
    return list(range(0, length, 2)) + list(range(1, length, 2))[::-1]


def ring_neighbours(col, count):
    odd = lax.rem(col, 2)
    even_next = col + 2 - (col + 2) // count
    odd_next = col - 2 + (count - col) // (count - 1)
    even_prev = col - 2 + 3 * ((count - col) // count)
    odd_prev = col + 2 - 3 * ((col + 1) // count)
    return (1 - odd) * even_next + odd * odd_next, (1 - odd) * even_prev + odd * odd_prev


def split(value):
    high = value.astype(jnp.bfloat16)
    return high, (value - high.astype(jnp.float32)).astype(jnp.bfloat16)


def kernel(
    row_count, col_count, groups,
    lower_ref, upper_ref, left_ref, piece_ref, out_ref,
    panel, lower_high, lower_low, upper_high, upper_low,
    x_high, x_low, half_high, half_low, solved, coupled, sums,
    gather_send, gather_recv, ring_send, ring_recv,
):
    row = lax.axis_index("row")
    col = lax.axis_index("col")
    ahead, behind = ring_neighbours(col, col_count)
    inner, width = piece_ref.shape
    rows = left_ref.shape[0] // col_count
    half = coupled.shape[2] // 2

    def swapped(bit):
        return (row + bit * (1 - 2 * lax.rem(row // bit, 2)), col)

    bits = []
    bit = row_count // 2
    while bit >= 1:
        bits.append(bit)
        bit //= 2
    targets = ((row, ahead), (row, behind))
    barrier = pltpu.get_barrier_semaphore()
    partners = [swapped(b) for b in bits] + list(targets)
    for partner in partners:
        pl.semaphore_signal(barrier, inc=1, device_id=partner, device_id_type=MESH)
    pl.semaphore_wait(barrier, len(partners))

    def held(mask):
        return piece_ref if mask == 0 else panel.at[mask - 1]

    def gather(mask):
        low = mask & -mask
        return pltpu.make_async_remote_copy(
            src_ref=held(mask ^ low), dst_ref=panel.at[mask - 1],
            send_sem=gather_send.at[mask - 1], recv_sem=gather_recv.at[mask - 1],
            device_id=swapped(low), device_id_type=MESH,
        )

    def pass_on(mask):
        for b in bits:
            if mask == 0 or b < (mask & -mask):
                gather(mask | b).start()

    def ring(group, side, step):
        if step == 0:
            slot = 0 if side == 0 else col_count - 2
            src = coupled.at[group, pl.ds(slot * rows, rows), pl.ds(side * half, half)]
        else:
            src = sums.at[group, side, step - 1]
        return pltpu.make_async_remote_copy(
            src_ref=src, dst_ref=sums.at[group, side, step],
            send_sem=ring_send.at[group, side, step], recv_sem=ring_recv.at[group, side, step],
            device_id=targets[side], device_id_type=MESH,
        )

    def begin(group):
        for side in range(2):
            ring(group, side, 0).start()

    def advance(group, step):
        last = step == col_count - 1
        for side in range(2):
            ring(group, side, step - 1).wait_recv()
            slot = step if last or side == 0 else col_count - 2 - step
            own = coupled[group, slot * rows:(slot + 1) * rows, side * half:(side + 1) * half]
            total = sums[group, side, step - 1] + own
            if last:
                at = group * 2 * half + side * half
                out_ref[:, at:at + half] = total
            else:
                sums[group, side, step - 1] = total
                ring(group, side, step).start()

    def tiles(count, body):
        def one(i, carry):
            body(pl.ds(pl.multiple_of(i * TILE, TILE), TILE))
            return carry

        lax.fori_loop(0, count // TILE, one, 0)

    def dot(a, b):
        return jnp.dot(a, b, preferred_element_type=jnp.float32)

    def three(a_high, a_low, b_high, b_low, at):
        high = a_high[at, :]
        return dot(high, b_high[...]) + (dot(high, b_low[...]) + dot(a_low[at, :], b_high[...]))

    def compute(group):
        for place, mask in enumerate(groups[group]):
            if mask:
                gather(mask).wait_recv()
                pass_on(mask)
        cols = [slice(place * width, (place + 1) * width) for place in range(len(groups[group]))]

        def cut(at):
            for place, mask in enumerate(groups[group]):
                high, low = split(held(mask)[at, :])
                x_high[at, cols[place]] = high
                x_low[at, cols[place]] = low

        tiles(inner, cut)

        def first(at):
            high, low = split(three(lower_high, lower_low, x_high, x_low, at))
            half_high[at, :] = high
            half_low[at, :] = low

        tiles(inner, first)

        def second(at):
            solved[at, :] = three(upper_high, upper_low, half_high, half_low, at).astype(jnp.bfloat16)

        tiles(inner, second)

        def third(at):
            coupled[group, at, :] = dot(left_ref[at, :], solved[...])

        tiles(left_ref.shape[0], third)

    pass_on(0)

    def factors(at):
        lower_high[at, :], lower_low[at, :] = split(lower_ref[at, :])
        upper_high[at, :], upper_low[at, :] = split(upper_ref[at, :])

    tiles(inner, factors)

    near = (len(groups) + 1) // 2
    done = {}
    for group in range(len(groups)):
        if group >= near:
            steps = col_count - 3 if group == near else col_count - 1
            for step in range(1, steps + 1):
                for other in range(near):
                    if done[other] < step:
                        advance(other, step)
                        done[other] = step
        compute(group)
        begin(group)
        done[group] = 0
    for step in range(1, col_count):
        for group in range(len(groups)):
            if done[group] < step:
                advance(group, step)
    for mask in range(1, row_count):
        gather(mask).wait_send()
    for group in range(len(groups)):
        for side in range(2):
            for step in range(col_count - 1):
                ring(group, side, step).wait_send()


def gather_solve_sum(lower_mat, upper_mat, left_mat, piece):
    row_count = lax.axis_size("row")
    col_count = lax.axis_size("col")
    inner, width = piece.shape
    per = max(1, GROUP_WIDTH // width)
    groups = [list(range(at, min(at + per, row_count))) for at in range(0, row_count, per)]
    wide = per * width
    count = len(groups)
    rows = left_mat.shape[0] // col_count
    bf16, f32 = jnp.bfloat16, jnp.float32
    dma = pltpu.SemaphoreType.DMA
    return pl.pallas_call(
        functools.partial(kernel, row_count, col_count, groups),
        out_shape=jax.ShapeDtypeStruct((rows, row_count * width), f32),
        in_specs=[pl.BlockSpec(memory_space=pltpu.VMEM)] * 4,
        out_specs=pl.BlockSpec(memory_space=pltpu.VMEM),
        scratch_shapes=[
            pltpu.VMEM((row_count - 1, inner, width), f32),
            pltpu.VMEM((inner, inner), bf16),
            pltpu.VMEM((inner, inner), bf16),
            pltpu.VMEM((inner, inner), bf16),
            pltpu.VMEM((inner, inner), bf16),
            pltpu.VMEM((inner, wide), bf16),
            pltpu.VMEM((inner, wide), bf16),
            pltpu.VMEM((inner, wide), bf16),
            pltpu.VMEM((inner, wide), bf16),
            pltpu.VMEM((inner, wide), bf16),
            pltpu.VMEM((count, left_mat.shape[0], wide), f32),
            pltpu.VMEM((count, 2, col_count - 1, rows, wide // 2), f32),
            dma((row_count - 1,)),
            dma((row_count - 1,)),
            dma((count, 2, col_count - 1)),
            dma((count, 2, col_count - 1)),
        ],
        compiler_params=pltpu.CompilerParams(
            collective_id=0, has_side_effects=True, vmem_limit_bytes=VMEM_LIMIT
        ),
    )(lower_mat, upper_mat, left_mat, piece)


def ring_rows(left_mat, block_ids, owners):
    block_count = block_ids.shape[0]
    shaped = left_mat.reshape(block_count, left_mat.shape[0] // block_count, left_mat.shape[1])
    placed = jnp.zeros((owners.shape[0],) + shaped.shape[1:], left_mat.dtype)
    for k in range(block_count):
        hit = (owners == block_ids[k])[:, None, None]
        placed = jnp.where(hit, shaped[k][None], placed)
    return placed.reshape(-1, left_mat.shape[1])


def per_device(
    lower_inverse, upper_inverse, left_coupling, right_pieces, interface_block, a_gg, panel_order
):
    row_count = lax.axis_size("row")
    col_count = lax.axis_size("col")
    order = ring_order(col_count)
    table = np.zeros((col_count, col_count), np.int32)
    for place, col in enumerate(order):
        for u in range(col_count):
            table[col, u] = order[(place - 1 - u) % col_count]
    owners = jnp.asarray(table)[lax.axis_index("col")]
    left_mat = ring_rows(left_coupling[0, 0], interface_block[0, 0], owners)
    width = right_pieces.shape[2]
    base = a_gg[0]
    total = gather_solve_sum(lower_inverse[0, 0], upper_inverse[0, 0], left_mat, right_pieces[0])
    me = lax.axis_index("row")
    positions = jnp.arange(row_count, dtype=jnp.int32)
    stored = jnp.sum((panel_order[:, None] == positions[None, :]).astype(jnp.int32) * positions[:, None], axis=0)
    stored = jnp.bitwise_xor(stored, me.astype(jnp.int32))
    columns = [
        base[:, b * width:(b + 1) * width]
        - lax.dynamic_slice(total, (0, stored[b] * width), (total.shape[0], width))
        for b in range(row_count)
    ]
    return jnp.concatenate(columns, axis=1)[None]


def solution(mesh):
    return jax.shard_map(
        per_device,
        mesh=mesh,
        in_specs=(
            P("row", "col", None, None),
            P("row", "col", None, None),
            P("row", "col", None, None),
            P("col", None, "row"),
            P("row", "col", None),
            P("row", "col", None),
            P(),
        ),
        out_specs=P("row", "col", None),
        check_vma=False,
    )
```
